8 devices in a mesh: batch: 1 (over z), row: 2 (over y), col: 4 (over x, core).
Axes of the slice: x: 2, y: 2, z: 1, core: 2. Of those that a mesh axis runs over, the one named last changes fastest.
Arguments:
- lower_mat: bfloat16 [4096, 4096], P('row', 'col')
- rhs_mat: bfloat16 [4096, 512], P('row', ('batch', 'col'))
Outputs:
- output: bfloat16 [4096, 512], P('row', ('batch', 'col'))
All inputs are finite; a program needn't handle non-finite values.
Results may differ from the reference program's by a relative error of at most 0.001.
Values are sent between devices in bfloat16 or wider.
A program may use at most 1 GiB of HBM per device.

```python
import jax
import jax.numpy as jnp
from jax import lax

MAT_ORDER = 4096
BLOCK_SIZE = 256
RHS_COLS = 512
GRID_ROWS = 2
GRID_COLS = 4


def stored_to_global(positions, grid_size):
    per_device = MAT_ORDER // grid_size
    device_idx = positions // per_device
    local_pos = positions % per_device
    return ((local_pos // BLOCK_SIZE) * grid_size + device_idx) * BLOCK_SIZE + local_pos % BLOCK_SIZE


def setup_inputs(seed: int = 0, part: int = 0) -> dict:
    key_mat, key_rhs = jax.random.split(jax.random.key(seed))
    col_global = stored_to_global(jnp.arange(MAT_ORDER), GRID_COLS)

    def draw_rows(block_idx):
        row_global = stored_to_global(block_idx * BLOCK_SIZE + jnp.arange(BLOCK_SIZE), GRID_ROWS)
        draws = jax.random.normal(jax.random.fold_in(key_mat, block_idx), (BLOCK_SIZE, MAT_ORDER), jnp.float32)
        scaled = draws / jnp.sqrt((row_global + 1).astype(jnp.float32))[:, None]
        keep = col_global[None, :] <= row_global[:, None]
        return jnp.where(keep, scaled, 0.0).astype(jnp.bfloat16)

    lower_mat = lax.map(draw_rows, jnp.arange(MAT_ORDER // BLOCK_SIZE)).reshape(MAT_ORDER, MAT_ORDER)
    rhs_mat = jax.random.normal(jax.random.fold_in(key_rhs, part), (MAT_ORDER, RHS_COLS), jnp.float32).astype(jnp.bfloat16)
    return {"lower_mat": lower_mat, "rhs_mat": rhs_mat}


def reference(lower_mat, rhs_mat):
    total_blocks = MAT_ORDER // BLOCK_SIZE
    row_blocks = total_blocks // GRID_ROWS
    col_blocks = total_blocks // GRID_COLS
    rhs_global = rhs_mat.reshape(GRID_ROWS, row_blocks, BLOCK_SIZE, RHS_COLS).transpose(1, 0, 2, 3).reshape(MAT_ORDER, RHS_COLS)
    outputs = []
    for stored_block in range(total_blocks):
        global_block = (stored_block % row_blocks) * GRID_ROWS + stored_block // row_blocks
        width = (global_block + 1) * BLOCK_SIZE
        row_panel = lower_mat[stored_block * BLOCK_SIZE:(stored_block + 1) * BLOCK_SIZE]
        panel_global = row_panel.reshape(BLOCK_SIZE, GRID_COLS, col_blocks, BLOCK_SIZE).transpose(0, 2, 1, 3).reshape(BLOCK_SIZE, MAT_ORDER)
        block_sum = jnp.dot(panel_global[:, :width], rhs_global[:width], preferred_element_type=jnp.float32)
        outputs.append(block_sum.astype(jnp.bfloat16))
    return jnp.concatenate(outputs, axis=0)
```

```python
import jax
import jax.numpy as jnp
from jax import lax
from jax.experimental import pallas as pl
from jax.experimental.pallas import tpu as pltpu
from jax.sharding import PartitionSpec as P

BLK = 256
RB = 8
CB = 4
MESH = pl.DeviceIdType.MESH


def kernel(l_hbm, b_hbm, out, lb, bs, bo, bc, bx, xl, own, psend, precv, x0,
           loc_sem, sxb, rxb, syo, ryo, sfw, rfw, spl, rpl, smx, rmx, sp, rp):
    r = lax.axis_index("row")
    col = lax.axis_index("col")
    x = col // 2
    core = col % 2
    xn = {"col": col + 2 - 4 * x}
    yn = {"row": 1 - r}
    pn = {"col": col + 1 - 2 * core}

    def rows(i, n=1):
        return pl.ds(i * BLK, n * BLK)

    def remote(src, dst, ssem, rsem, dev):
        return pltpu.make_async_remote_copy(
            src_ref=src, dst_ref=dst, send_sem=ssem, recv_sem=rsem, device_id=dev, device_id_type=MESH)

    barrier = pltpu.get_barrier_semaphore()
    for dev in (xn, yn, pn):
        pl.semaphore_signal(barrier, inc=1, device_id=dev, device_id_type=MESH)

    loads = []
    for t in range(CB):
        loads.append((b_hbm.at[rows(2 * t + 1 - x)], bs.at[rows(t)]))
    for t in range(CB):
        loads.append((b_hbm.at[rows(2 * t + x)], bo.at[r, rows(t)]))
    loads.append((b_hbm.at[rows(1 - x)], bx.at[r]))
    for u in range(CB):
        part = (rows(2 * u, 2), pl.ds(0, (u + 1) * BLK))
        loads.append((l_hbm.at[part], lb.at[(core,) + part]))
    loads = [pltpu.make_async_copy(s, d, loc_sem.at[i]) for i, (s, d) in enumerate(loads)]
    for cp in loads:
        cp.start()
    for cp in loads:
        cp.wait()

    x_b = [remote(bs.at[rows(t)], bc.at[r, rows(t)], sxb.at[t], rxb.at[t], xn) for t in range(CB)]
    y_own = [remote(bo.at[r, rows(t)], bo.at[r, rows(t)], syo.at[t], ryo.at[t], yn) for t in range(CB)]
    y_bx = remote(bx.at[r], bx.at[r], syo.at[CB], ryo.at[CB], yn)
    y_fwd = [remote(bc.at[r, rows(t)], bc.at[r, rows(t)], sfw.at[t], rfw.at[t], yn) for t in range(CB)]
    p_l = []
    for u in range(CB):
        part = (core, rows(2 * u, 2), pl.ds(0, (u + 1) * BLK))
        p_l.append(remote(lb.at[part], lb.at[part], spl.at[u], rpl.at[u], pn))
    x_l = [remote(lb.at[core, rows(j + 1), pl.ds(0, BLK)], xl.at[core, j], smx.at[j], rmx.at[j], xn) for j in range(2)]
    p_xl = [remote(xl.at[core, j], xl.at[core, j], smx.at[2 + j], rmx.at[2 + j], pn) for j in range(2)]
    x_0 = remote(x0.at[0], x0.at[1], smx.at[4], rmx.at[4], xn)
    x_p = {s: remote(psend.at[s - 2], precv.at[s - 2], sp.at[s - 2], rp.at[s - 2], xn) for s in range(2, RB)}

    left = x == 0
    right = x == 1
    sends_l1 = (r == 1) | (x == 0) | (core == 0)
    gets_l1 = (r == 1) | (x == 1) | (core == 0)
    partner_gets_l1 = (r == 1) | (x == 1) | (core == 1)

    pl.semaphore_wait(barrier, 3)

    for cp in x_b + y_own[:3] + p_l:
        cp.start()
    pl.when(sends_l1)(x_l[0].start)
    pl.when(right)(x_l[1].start)

    for t in range(CB):
        x_b[t].wait_recv()
        y_fwd[t].start()
        if t == 2:
            y_own[3].start()
    y_bx.start()

    def product(s, cross):
        k = (s // 2 + 1) * BLK
        total = None
        for p in range(2):
            rhs = bo[p, :k, :]
            if cross:
                rhs = jnp.concatenate([rhs, bc[p, :k, :]], axis=1)
            term = jnp.dot(lb[p, s * BLK:(s + 1) * BLK, :k], rhs, preferred_element_type=jnp.float32)
            total = term if total is None else total + term
        return total

    for t in range(CB):
        y_own[t].wait_recv()
        y_fwd[t].wait_recv()
        p_l[t].wait_recv()
        for s in (2 * t, 2 * t + 1):
            if s == 0:
                @pl.when(left)
                def _():
                    total = product(0, True)
                    x0[0, :, :] = total[:, 128:].astype(jnp.bfloat16)
                    out[0:BLK, :] = total[:, :128].astype(jnp.bfloat16)
                    x_0.start()
            elif s == 1:
                own[1] = product(1, False)
            else:
                total = product(s, True)
                psend[s - 2] = total[:, 128:]
                own[s] = total[:, :128]
                if s == 2:
                    pl.when(left)(x_p[s].start)
                else:
                    x_p[s].start()

    @pl.when(gets_l1)
    def _():
        x_l[0].wait_recv()
        p_xl[0].start()

    @pl.when(left)
    def _():
        x_l[1].wait_recv()
        p_xl[1].start()

    y_bx.wait_recv()
    pl.when(partner_gets_l1)(p_xl[0].wait_recv)

    @pl.when((r == 1) | right)
    def _():
        own[1] += jnp.dot(xl[1, 0], bx[1], preferred_element_type=jnp.float32)

    out[BLK:2 * BLK, :] = (own[1] + jnp.dot(xl[0, 0], bx[0], preferred_element_type=jnp.float32)).astype(jnp.bfloat16)

    @pl.when(left)
    def _():
        p_xl[1].wait_recv()
        total = own[2]
        for p in range(2):
            total += jnp.dot(xl[p, 1], bx[p], preferred_element_type=jnp.float32)
        out[2 * BLK:3 * BLK, :] = total.astype(jnp.bfloat16)

    @pl.when(right)
    def _():
        x_0.wait_recv()
        out[0:BLK, :] = x0[1]
        x_p[2].wait_recv()
        out[2 * BLK:3 * BLK, :] = (own[2] + precv[0]).astype(jnp.bfloat16)

    for s in range(3, RB):
        x_p[s].wait_recv()
        out[s * BLK:(s + 1) * BLK, :] = (own[s] + precv[s - 2]).astype(jnp.bfloat16)

    for cp in x_b + y_own + [y_bx] + y_fwd + p_l + [x_p[s] for s in range(3, RB)]:
        cp.wait_send()
    pl.when(sends_l1)(x_l[0].wait_send)
    pl.when(gets_l1)(p_xl[0].wait_send)
    pl.when(right)(x_l[1].wait_send)

    @pl.when(left)
    def _():
        p_xl[1].wait_send()
        x_0.wait_send()
        x_p[2].wait_send()


def solution(mesh):
    def local_product(lower_loc, rhs_loc):
        n_rows, cols = rhs_loc.shape
        depth = lower_loc.shape[1]
        bf, f32 = jnp.bfloat16, jnp.float32
        dma = pltpu.SemaphoreType.DMA
        return pl.pallas_call(
            kernel,
            out_shape=jax.ShapeDtypeStruct((n_rows, cols), bf),
            in_specs=[pl.BlockSpec(memory_space=pltpu.HBM)] * 2,
            out_specs=pl.BlockSpec(memory_space=pltpu.VMEM),
            scratch_shapes=[
                pltpu.VMEM((2, n_rows, depth), bf),
                pltpu.VMEM((depth, cols), bf),
                pltpu.VMEM((2, depth, cols), bf),
                pltpu.VMEM((2, depth, cols), bf),
                pltpu.VMEM((2, BLK, cols), bf),
                pltpu.VMEM((2, 2, BLK, BLK), bf),
                pltpu.VMEM((RB, BLK, cols), f32),
                pltpu.VMEM((RB - 2, BLK, cols), f32),
                pltpu.VMEM((RB - 2, BLK, cols), f32),
                pltpu.VMEM((2, BLK, cols), bf),
                dma((3 * CB + 1,)),
                dma((CB,)), dma((CB,)),
                dma((CB + 1,)), dma((CB + 1,)),
                dma((CB,)), dma((CB,)),
                dma((CB,)), dma((CB,)),
                dma((5,)), dma((5,)),
                dma((RB - 2,)), dma((RB - 2,)),
            ],
            compiler_params=pltpu.CompilerParams(
                collective_id=0, has_side_effects=True, vmem_limit_bytes=32 * 2**20),
        )(lower_loc, rhs_loc)

    return jax.shard_map(local_product, mesh=mesh, in_specs=(P("row", "col"), P("row", ("batch", "col"))), out_specs=P("row", ("batch", "col")), check_vma=False)
```
